256 devices in a mesh: replica: 32 (over y, z), expert: 8 (over x, core).
Axes of the slice: x: 4, y: 4, z: 8, core: 2. Of those that a mesh axis runs over, the one named last changes fastest.
Arguments:
- outer_params: float32 [28672, 4096], P('expert', 'replica'), may hold values from -6 to 6
- momentum: bfloat16 [28672, 4096], P('expert', 'replica'), may hold values from -6 to 6
- replica_deltas: bfloat16 [32, 16, 128, 4096], P('replica', 'expert'), may hold values from -6 to 6
- replica_rows: bfloat16 [32, 16, 128, 4096], P('replica', 'expert'), may hold values from -6 to 6
- block_ids: int32 [32, 16], P('replica', 'expert'), may hold values from 0 to 223, as said below
- slot_counts: int32 [32, 8], P('replica', 'expert'), may hold values from 0 to 2, as said below
Outputs:
- new_params: float32 [28672, 4096], P('expert', 'replica')
- new_momentum: bfloat16 [28672, 4096], P('expert', 'replica')
- blended_rows: bfloat16 [32, 16, 128, 4096], P('replica', 'expert')
The draws below stay inside these ranges and needn't reach their ends.
Inputs may be any that keep to these rules, and one draw needn't show every extreme that they name: `block_ids`: within row r, slots e * 2 to (e + 1) * 2 - 1 name distinct blocks among e * 28 to (e + 1) * 28 - 1. The first slot_counts[r, e] slots of group e of row r are live, the rest are padding; in every draw some index e has 2 in every row.
All inputs are finite; a program needn't handle non-finite values.
Results may differ from the reference program's by a relative error of at most 0.0075.
Values may be sent and summed in bfloat16 or wider, within the bound.
A program may use at most 64 MiB of HBM per device.

```python
import jax
import jax.numpy as jnp
from jax import lax

D = 4096
BLOCK = 128
MAXB = 2
REPLICAS = 32
ROWS = 28672
LB = 28
SLOTS = 16
N_EXPERT = 8


def draw_block_ids(key, part):
    scores = jax.random.randint(jax.random.fold_in(key, 11), (REPLICAS, N_EXPERT, LB), 0, 1048576)
    scores = scores * LB + jnp.arange(LB, dtype=jnp.int32)[None, None, :]
    order = jnp.argsort(scores, axis=2, stable=True)[:, :, :MAXB].astype(jnp.int32)
    offsets = (jnp.arange(N_EXPERT, dtype=jnp.int32) * LB)[None, :, None]
    return (order + offsets).reshape(REPLICAS, N_EXPERT * MAXB)


def draw_slot_counts(key, part):
    counts = jax.random.randint(jax.random.fold_in(key, 23), (REPLICAS, N_EXPERT), 0, MAXB + 1)
    hottest = jax.random.randint(jax.random.fold_in(key, 37), (), 0, N_EXPERT)
    column = jnp.arange(N_EXPERT, dtype=jnp.int32)[None, :]
    return jnp.where(column == hottest, MAXB, counts).astype(jnp.int32)


def steps_of(key, shape, pieces, smallest, top_value):
    factor_of = 1.0
    for position, blocks in pieces:
        draws = jax.random.uniform(jax.random.fold_in(jax.random.fold_in(key, 6), position), (blocks,), jnp.float32, smallest / len(pieces), top_value / len(pieces))
        factor_of = factor_of * jnp.repeat(jnp.exp(draws), shape[position] // blocks).reshape((-1,) + (1,) * (len(shape) - 1 - position))
    return factor_of


def noise(rng, shape, spread, limit, split=(), kind=jnp.bfloat16):
    factor_of = steps_of(rng, shape, split, -0.22, 0.18) if split else 1.0
    drawn = jax.random.normal(rng, shape, jnp.float32) * spread * factor_of
    return jnp.minimum(jnp.maximum(drawn, -limit), limit).astype(kind)


def setup_inputs(seed: int = 0) -> dict:
    key_list = jax.random.split(jax.random.key(seed), 7)
    outer_params = noise(key_list[0], (ROWS, D), 1.0, 6.0, ((0, 8), (1, 32)), jnp.float32)
    momentum = noise(key_list[1], (ROWS, D), 1.0, 6.0, ((0, 8), (1, 32)))
    replica_deltas = noise(key_list[2], (REPLICAS, SLOTS, BLOCK, D), 1.0, 6.0, ((0, 32), (1, 8)))
    replica_rows = noise(key_list[3], (REPLICAS, SLOTS, BLOCK, D), 1.0, 6.0, ((0, 32), (1, 8)))
    block_ids = draw_block_ids(jax.random.fold_in(key_list[6], 71), 0)
    slot_counts = draw_slot_counts(jax.random.fold_in(key_list[6], 71), 0)
    return {"outer_params": outer_params, "momentum": momentum, "replica_deltas": replica_deltas, "replica_rows": replica_rows, "block_ids": block_ids, "slot_counts": slot_counts}


outer_rate = 0.7
nesterov_decay = 0.9
blend_weight = 0.5


def reference(outer_params, momentum, replica_deltas, replica_rows, block_ids, slot_counts):
    block_total = ROWS // BLOCK
    slot_index = jnp.arange(SLOTS, dtype=jnp.int32) % MAXB
    group_index = jnp.arange(SLOTS, dtype=jnp.int32) // MAXB
    active = slot_index[None, :] < slot_counts[:, group_index]

    def accumulate(carry, inputs):
        totals, tallies = carry
        deltas, listed, flags = inputs
        weights = flags.astype(jnp.float32)
        totals = totals.at[listed].add(deltas.astype(jnp.float32) * weights[:, None, None])
        tallies = tallies.at[listed].add(weights)
        return (totals, tallies), None

    start = (jnp.zeros((block_total, BLOCK, D), jnp.float32), jnp.zeros((block_total,), jnp.float32))
    (totals, tallies), unused = lax.scan(accumulate, start, (replica_deltas, block_ids, active))
    mean_delta = (totals / jnp.maximum(tallies, 1.0)[:, None, None]).reshape(ROWS, D)
    moment = nesterov_decay * momentum.astype(jnp.float32) + mean_delta
    params_new = outer_params - outer_rate * (mean_delta + nesterov_decay * moment)
    blocks_new = params_new.reshape(block_total, BLOCK, D)

    def blend_one(inputs):
        rows, listed, flags = inputs
        fetched = lax.optimization_barrier(blocks_new[listed].astype(jnp.bfloat16)).astype(jnp.float32)
        rows_float = rows.astype(jnp.float32)
        mixed = blend_weight * rows_float + (1.0 - blend_weight) * fetched
        return jnp.where(flags[:, None, None], mixed, rows_float).astype(jnp.bfloat16)

    blended = lax.map(blend_one, (replica_rows, block_ids, active))
    return params_new, moment.astype(jnp.bfloat16), blended
```

```python
import functools

import jax
import jax.numpy as jnp
from jax import lax
from jax.experimental import pallas as pl
from jax.experimental.pallas import tpu as pltpu
from jax.sharding import PartitionSpec as P

outer_rate = 0.7
nesterov_decay = 0.9
blend_weight = 0.5

MESH = pl.DeviceIdType.MESH
TILE = 16
LANES = 128
RING = 8


def peer_at(k, me, n):
    kz = lax.rem(k, RING)
    far = lax.div(kz + 1, 2) * (1 - 2 * lax.rem(kz + 1, 2))
    z = lax.rem(lax.rem(me, RING) + far + RING, RING)
    y = lax.rem(lax.div(me, RING) + lax.div(k, RING), n // RING)
    return y * RING + z


def kernel(
    n, chunks, blocks,
    ids_ref, count_ref, deltas_ref, rows_ref, params_ref, momentum_ref,
    params, momentum, own,
    src, got, sel, tally, fresh, back, ret, mine, table, listed, own_ids, own_count,
    local_sem, table_sem, table_send, list_sem, send1, recv1, send2, recv2,
):
    me = lax.axis_index("replica")
    slots = src.shape[0]
    block = src.shape[1]
    rows = block // chunks
    tiles = rows // TILE
    total = n * slots
    loads = [
        pltpu.make_async_copy(a, b, local_sem.at[i])
        for i, (a, b) in enumerate(
            (
                (ids_ref, own_ids), (count_ref, own_count), (deltas_ref.at[0], src),
                (params_ref, params), (momentum_ref, momentum), (rows_ref, own),
            )
        )
    ]
    for copy in loads:
        copy.start()

    barrier = pltpu.get_barrier_semaphore()

    @pl.loop(1, n)
    def _(k):
        pl.semaphore_signal(barrier, inc=1, device_id={"replica": peer_at(k, me, n)}, device_id_type=MESH)

    loads[0].wait()
    loads[1].wait()
    first = lax.axis_index("expert") * blocks
    count = own_count[0, 0]
    lane = lax.broadcasted_iota(jnp.int32, (1, LANES), 1)
    row = jnp.full((1, LANES), -1, jnp.int32)
    for j in range(slots):
        row = jnp.where((lane == j) & (j < count), own_ids[0, j] - first, row)
    mine[...] = row
    table[me] = row
    loads[2].wait()
    pl.semaphore_wait(barrier, n - 1)

    def cols(p):
        return pl.ds(pl.multiple_of(p * LANES, LANES), LANES)

    @pl.loop(1, n)
    def _(k):
        p = peer_at(k, me, n)
        pltpu.make_async_remote_copy(
            src_ref=mine, dst_ref=table.at[me], send_sem=table_send, recv_sem=table_sem,
            device_id={"replica": p}, device_id_type=MESH,
        ).start()

    @pl.loop(0, chunks)
    def _(c):
        part = pl.ds(c * rows, rows)

        @pl.loop(1, n)
        def _(k):
            p = peer_at(k, me, n)
            pltpu.make_async_remote_copy(
                src_ref=src.at[:, part, cols(p)], dst_ref=got.at[c, me], send_sem=send1, recv_sem=recv1.at[c],
                device_id={"replica": p}, device_id_type=MESH,
            ).start()

    for c in range(chunks):
        got[c, me] = src[:, c * rows : (c + 1) * rows, cols(me)]

    rest = table.at[pl.ds(0, n - 1)]
    pltpu.make_async_copy(rest, rest, table_sem).wait()
    to_scalars = pltpu.make_async_copy(table, listed, list_sem)
    to_scalars.start()
    to_scalars.wait()
    slot_of = lax.broadcasted_iota(jnp.int32, (1, total * TILE), 1)
    inner = lax.rem(slot_of, TILE)
    slot_of = lax.div(slot_of, TILE)
    target = jnp.full((1, total * TILE), -TILE, jnp.int32)
    for s in range(total):
        target = jnp.where(slot_of == s, listed[s // slots, 0, s % slots] * TILE, target)
    target = target + inner
    at = lax.broadcasted_iota(jnp.int32, (TILE, total * TILE), 0)

    @pl.loop(0, blocks)
    def _(b):
        there = pl.ds(pl.multiple_of(b * TILE, TILE), TILE)
        sel[there, :] = jnp.where(at + b * TILE == target, 1.0, 0.0).astype(jnp.bfloat16)

    tally[...] = jnp.maximum(
        jnp.dot(sel[...], jnp.ones((total * TILE, LANES), jnp.bfloat16), preferred_element_type=jnp.float32), 1.0
    )
    loads[3].wait()
    loads[4].wait()

    @pl.loop(0, chunks)
    def _(c):
        arrived = got.at[c, pl.ds(0, n - 1)]
        pltpu.make_async_copy(arrived, arrived, recv1.at[c]).wait()

        @pl.loop(0, tiles)
        def _(t):
            inside = pl.ds(pl.multiple_of(t * TILE, TILE), TILE)
            here = pl.ds(pl.multiple_of(c * rows + t * TILE, TILE), TILE)
            tile = got[c, :, :, inside, :].reshape(total * TILE, LANES)
            totals = jnp.dot(sel[...], tile, preferred_element_type=jnp.float32)
            mean = totals / tally[...]
            moment = nesterov_decay * momentum[:, here, :].reshape(blocks * TILE, LANES).astype(jnp.float32) + mean
            fresh_tile = params[:, here, :].reshape(blocks * TILE, LANES) - outer_rate * (
                mean + nesterov_decay * moment
            )
            params[:, here, :] = fresh_tile.reshape(blocks, TILE, LANES)
            momentum[:, here, :] = moment.astype(jnp.bfloat16).reshape(blocks, TILE, LANES)
            fresh[:, inside, :] = fresh_tile.astype(jnp.bfloat16).reshape(blocks, TILE, LANES)

        part = pl.ds(pl.multiple_of(c * rows, TILE), rows)
        for s in range(total):
            back[c, s // slots, s % slots] = fresh[jnp.maximum(listed[s // slots, 0, s % slots], 0)]

        for j in range(slots):
            ret[j, part, cols(me)] = fresh[jnp.maximum(listed[me, 0, j], 0)]

        @pl.loop(1, n)
        def _(k):
            p = peer_at(k, me, n)
            pltpu.make_async_remote_copy(
                src_ref=back.at[c, p], dst_ref=ret.at[:, part, cols(me)], send_sem=send2, recv_sem=recv2.at[c],
                device_id={"replica": p}, device_id_type=MESH,
            ).start()

    loads[5].wait()

    @pl.loop(0, chunks)
    def _(c):
        arrived = got.at[c, pl.ds(0, n - 1)]
        pltpu.make_async_copy(arrived, arrived, recv2.at[c]).wait()
        part = pl.ds(pl.multiple_of(c * rows, TILE), rows)
        for j in range(slots):

            @pl.loop(0, n)
            def _(q):
                old = own[0, j, part, cols(q)].astype(jnp.float32)
                new = ret[j, part, cols(q)].astype(jnp.float32)
                mixed = blend_weight * old + (1.0 - blend_weight) * new
                own[0, j, part, cols(q)] = jnp.where(j < count, mixed, old).astype(jnp.bfloat16)


    pltpu.make_async_copy(rest, rest, table_send).wait()
    sent = got.at[:, pl.ds(0, n - 1)]
    pltpu.make_async_copy(sent, sent, send1).wait()
    pltpu.make_async_copy(sent, sent, send2).wait()


def write_out(params, momentum, own, params_out, momentum_out, blended_out, sem):
    copies = [
        pltpu.make_async_copy(a, b, sem.at[i])
        for i, (a, b) in enumerate(((params, params_out), (own, blended_out), (momentum, momentum_out)))
    ]
    for copy in copies:
        copy.start()
    for copy in copies:
        copy.wait()


def local(outer_params, momentum, replica_deltas, replica_rows, block_ids, slot_counts):
    n = lax.axis_size("replica")
    _, slots, block, width = replica_deltas.shape
    blocks = outer_params.shape[0] // block
    slab = outer_params.shape[1]
    total = n * slots
    chunks = 4
    rows = block // chunks
    f32, bf16 = jnp.float32, jnp.bfloat16
    hbm = pl.BlockSpec(memory_space=pltpu.HBM)
    vmem = pl.BlockSpec(memory_space=pltpu.VMEM)
    dma = pltpu.SemaphoreType.DMA
    results = (
        jax.ShapeDtypeStruct((blocks, block, slab), f32),
        jax.ShapeDtypeStruct((blocks, block, slab), bf16),
        jax.ShapeDtypeStruct(replica_rows.shape, bf16),
    )
    held = pl.pallas_call(
        functools.partial(kernel, n, chunks, blocks),
        out_shape=results,
        in_specs=[hbm] * 6,
        out_specs=(vmem,) * 3,
        scratch_shapes=[
            pltpu.VMEM((slots, block, width), bf16),
            pltpu.VMEM((chunks, n, slots, rows, slab), bf16),
            pltpu.VMEM((blocks * TILE, total * TILE), bf16),
            pltpu.VMEM((blocks * TILE, slab), f32),
            pltpu.VMEM((blocks, rows, slab), bf16),
            pltpu.VMEM((chunks, n, slots, rows, slab), bf16),
            pltpu.VMEM((slots, block, width), bf16),
            pltpu.VMEM((1, LANES), jnp.int32),
            pltpu.VMEM((n, 1, LANES), jnp.int32),
            pltpu.SMEM((n, 1, LANES), jnp.int32),
            pltpu.SMEM((1, slots), jnp.int32),
            pltpu.SMEM((1, 1), jnp.int32),
            dma((6,)), dma, dma, dma, dma, dma((chunks,)), dma, dma((chunks,)),
        ],
        compiler_params=pltpu.CompilerParams(
            collective_id=0, has_side_effects=True, vmem_limit_bytes=32 * 1024 * 1024
        ),
        cost_estimate=pl.CostEstimate(flops=10**9, bytes_accessed=13 * 10**6, transcendentals=0),
    )(
        *(
            pltpu.with_memory_space_constraint(a, pltpu.HBM) if a.size > 1 else a
            for a in (
                block_ids, slot_counts, replica_deltas, replica_rows,
                outer_params.reshape(blocks, block, slab), momentum.reshape(blocks, block, slab),
            )
        ),
    )
    new_params, new_momentum, blended = pl.pallas_call(
        write_out,
        out_shape=results,
        in_specs=[vmem] * 3,
        out_specs=(hbm,) * 3,
        scratch_shapes=[dma((3,))],
        compiler_params=pltpu.CompilerParams(vmem_limit_bytes=16 * 1024 * 1024),
    )(*held)
    return new_params.reshape(outer_params.shape), new_momentum.reshape(momentum.shape), blended


def solution(mesh):
    in_specs = (
        P("expert", "replica"),
        P("expert", "replica"),
        P("replica", "expert", None, None),
        P("replica", "expert", None, None),
        P("replica", "expert"),
        P("replica", "expert"),
    )
    out_specs = (P("expert", "replica"), P("expert", "replica"), P("replica", "expert", None, None))
    return jax.shard_map(local, mesh=mesh, in_specs=in_specs, out_specs=out_specs, check_vma=False)
```

```python
import functools

import jax
import jax.numpy as jnp
from jax import lax
from jax.experimental import pallas as pl
from jax.experimental.pallas import tpu as pltpu
from jax.sharding import PartitionSpec as P

outer_rate = 0.7
nesterov_decay = 0.9
blend_weight = 0.5

MESH = pl.DeviceIdType.MESH
TILE = 16
LANES = 128
RING = 8


GROUPS = 5


def peer_in(g, i, me, n):
    if g == 0:
        dy, dz = i + 1, 0
    elif g == GROUPS - 1:
        dy, dz = i, g
    else:
        dy, dz = lax.div(i, 2), g * (1 - 2 * lax.rem(i, 2))
    z = lax.rem(lax.rem(me, RING) + dz + RING, RING)
    y = lax.rem(lax.div(me, RING) + dy, n // RING)
    return y * RING + z


def group_size(g, n):
    return (n // RING - 1, 2 * (n // RING), 2 * (n // RING), 2 * (n // RING), n // RING)[g]


def kernel(
    n, chunks, blocks,
    ids_ref, count_ref, deltas_ref, rows_ref, params_ref, momentum_ref,
    params, momentum, own,
    src, got, sel, tally, fresh, back, ret, mine, table, listed, own_ids, own_count,
    local_sem, known, table_sem, table_send, list_sem, send1, recv1, send2, recv2,
):
    me = lax.axis_index("replica")
    slots = src.shape[0]
    block = src.shape[1]
    rows = block // chunks
    tiles = rows // TILE
    total = n * slots
    loads = [
        pltpu.make_async_copy(a, b, local_sem.at[i])
        for i, (a, b) in enumerate(
            (
                (ids_ref, own_ids), (count_ref, own_count), (deltas_ref.at[0], src),
                (params_ref, params), (momentum_ref, momentum), (rows_ref, own),
            )
        )
    ]
    for copy in loads:
        copy.start()

    barrier = pltpu.get_barrier_semaphore()

    for g in (0, 1):

        @pl.loop(0, group_size(g, n))
        def _(i):
            pl.semaphore_signal(
                barrier, inc=1, device_id={"replica": peer_in(g, i, me, n)}, device_id_type=MESH
            )

    loads[0].wait()
    loads[1].wait()
    first = lax.axis_index("expert") * blocks
    count = own_count[0, 0]
    lane = lax.broadcasted_iota(jnp.int32, (1, LANES), 1)
    row = jnp.full((1, LANES), -1, jnp.int32)
    for j in range(slots):
        row = jnp.where((lane == j) & (j < count), own_ids[0, j] - first, row)
    mine[...] = row
    table[me] = row
    loads[2].wait()
    pl.semaphore_wait(barrier, group_size(0, n) + group_size(1, n))

    def cols(p):
        return pl.ds(pl.multiple_of(p * LANES, LANES), LANES)

    def tell(level):
        for away in (1, RING - 1):
            z = lax.rem(lax.rem(me, RING) + away, RING)
            pl.semaphore_signal(
                known.at[level], inc=1, device_id={"replica": lax.div(me, RING) * RING + z}, device_id_type=MESH
            )

    def send_table(g):
        @pl.loop(0, group_size(g, n))
        def _(i):
            pltpu.make_async_remote_copy(
                src_ref=mine, dst_ref=table.at[me], send_sem=table_send, recv_sem=table_sem,
                device_id={"replica": peer_in(g, i, me, n)}, device_id_type=MESH,
            ).start()

    def send_slab(c, g):
        part = pl.ds(c * rows, rows)

        @pl.loop(0, group_size(g, n))
        def _(i):
            p = peer_in(g, i, me, n)
            pltpu.make_async_remote_copy(
                src_ref=src.at[:, part, cols(p)], dst_ref=got.at[c, me], send_sem=send1, recv_sem=recv1.at[c],
                device_id={"replica": p}, device_id_type=MESH,
            ).start()

    for g in range(GROUPS):
        if g > 1:
            pl.semaphore_wait(known.at[g - 2], 2)
        if 0 < g < GROUPS - 1:
            tell(g - 1)
        send_table(g)
        send_slab(0, g)

    @pl.loop(1, chunks)
    def _(c):
        for g in range(GROUPS):
            send_slab(c, g)

    for c in range(chunks):
        got[c, me] = src[:, c * rows : (c + 1) * rows, cols(me)]

    rest = table.at[pl.ds(0, n - 1)]
    pltpu.make_async_copy(rest, rest, table_sem).wait()
    to_scalars = pltpu.make_async_copy(table, listed, list_sem)
    to_scalars.start()
    to_scalars.wait()
    slot_of = lax.broadcasted_iota(jnp.int32, (1, total * TILE), 1)
    inner = lax.rem(slot_of, TILE)
    slot_of = lax.div(slot_of, TILE)
    target = jnp.full((1, total * TILE), -TILE, jnp.int32)
    for s in range(total):
        target = jnp.where(slot_of == s, listed[s // slots, 0, s % slots] * TILE, target)
    target = target + inner
    at = lax.broadcasted_iota(jnp.int32, (TILE, total * TILE), 0)

    @pl.loop(0, blocks)
    def _(b):
        there = pl.ds(pl.multiple_of(b * TILE, TILE), TILE)
        sel[there, :] = jnp.where(at + b * TILE == target, 1.0, 0.0).astype(jnp.bfloat16)

    tally[...] = jnp.maximum(
        jnp.dot(sel[...], jnp.ones((total * TILE, LANES), jnp.bfloat16), preferred_element_type=jnp.float32), 1.0
    )
    loads[3].wait()
    loads[4].wait()

    @pl.loop(0, chunks)
    def _(c):
        arrived = got.at[c, pl.ds(0, n - 1)]
        pltpu.make_async_copy(arrived, arrived, recv1.at[c]).wait()

        @pl.loop(0, tiles)
        def _(t):
            inside = pl.ds(pl.multiple_of(t * TILE, TILE), TILE)
            here = pl.ds(pl.multiple_of(c * rows + t * TILE, TILE), TILE)
            tile = got[c, :, :, inside, :].reshape(total * TILE, LANES)
            totals = jnp.dot(sel[...], tile, preferred_element_type=jnp.float32)
            mean = totals / tally[...]
            moment = nesterov_decay * momentum[:, here, :].reshape(blocks * TILE, LANES).astype(jnp.float32) + mean
            fresh_tile = params[:, here, :].reshape(blocks * TILE, LANES) - outer_rate * (
                mean + nesterov_decay * moment
            )
            params[:, here, :] = fresh_tile.reshape(blocks, TILE, LANES)
            momentum[:, here, :] = moment.astype(jnp.bfloat16).reshape(blocks, TILE, LANES)
            fresh[:, inside, :] = fresh_tile.astype(jnp.bfloat16).reshape(blocks, TILE, LANES)

        part = pl.ds(pl.multiple_of(c * rows, TILE), rows)
        for s in range(total):
            back[c, s // slots, s % slots] = fresh[jnp.maximum(listed[s // slots, 0, s % slots], 0)]

        for j in range(slots):
            ret[j, part, cols(me)] = fresh[jnp.maximum(listed[me, 0, j], 0)]

        for g in reversed(range(GROUPS)):

            @pl.loop(0, group_size(g, n))
            def _(i):
                p = peer_in(g, i, me, n)
                pltpu.make_async_remote_copy(
                    src_ref=back.at[c, p], dst_ref=ret.at[:, part, cols(me)], send_sem=send2, recv_sem=recv2.at[c],
                    device_id={"replica": p}, device_id_type=MESH,
                ).start()

    loads[5].wait()

    @pl.loop(0, chunks)
    def _(c):
        arrived = got.at[c, pl.ds(0, n - 1)]
        pltpu.make_async_copy(arrived, arrived, recv2.at[c]).wait()
        part = pl.ds(pl.multiple_of(c * rows, TILE), rows)
        for j in range(slots):

            @pl.loop(0, n)
            def _(q):
                old = own[0, j, part, cols(q)].astype(jnp.float32)
                new = ret[j, part, cols(q)].astype(jnp.float32)
                mixed = blend_weight * old + (1.0 - blend_weight) * new
                own[0, j, part, cols(q)] = jnp.where(j < count, mixed, old).astype(jnp.bfloat16)


    pltpu.make_async_copy(rest, rest, table_send).wait()
    sent = got.at[:, pl.ds(0, n - 1)]
    pltpu.make_async_copy(sent, sent, send1).wait()
    pltpu.make_async_copy(sent, sent, send2).wait()


def write_out(params, momentum, own, params_out, momentum_out, blended_out, sem):
    copies = [
        pltpu.make_async_copy(a, b, sem.at[i])
        for i, (a, b) in enumerate(((params, params_out), (own, blended_out), (momentum, momentum_out)))
    ]
    for copy in copies:
        copy.start()
    for copy in copies:
        copy.wait()


def local(outer_params, momentum, replica_deltas, replica_rows, block_ids, slot_counts):
    n = lax.axis_size("replica")
    _, slots, block, width = replica_deltas.shape
    blocks = outer_params.shape[0] // block
    slab = outer_params.shape[1]
    total = n * slots
    chunks = 2
    rows = block // chunks
    f32, bf16 = jnp.float32, jnp.bfloat16
    hbm = pl.BlockSpec(memory_space=pltpu.HBM)
    vmem = pl.BlockSpec(memory_space=pltpu.VMEM)
    dma = pltpu.SemaphoreType.DMA
    results = (
        jax.ShapeDtypeStruct((blocks, block, slab), f32),
        jax.ShapeDtypeStruct((blocks, block, slab), bf16),
        jax.ShapeDtypeStruct(replica_rows.shape, bf16),
    )
    held = pl.pallas_call(
        functools.partial(kernel, n, chunks, blocks),
        out_shape=results,
        in_specs=[hbm] * 6,
        out_specs=(vmem,) * 3,
        scratch_shapes=[
            pltpu.VMEM((slots, block, width), bf16),
            pltpu.VMEM((chunks, n, slots, rows, slab), bf16),
            pltpu.VMEM((blocks * TILE, total * TILE), bf16),
            pltpu.VMEM((blocks * TILE, slab), f32),
            pltpu.VMEM((blocks, rows, slab), bf16),
            pltpu.VMEM((chunks, n, slots, rows, slab), bf16),
            pltpu.VMEM((slots, block, width), bf16),
            pltpu.VMEM((1, LANES), jnp.int32),
            pltpu.VMEM((n, 1, LANES), jnp.int32),
            pltpu.SMEM((n, 1, LANES), jnp.int32),
            pltpu.SMEM((1, slots), jnp.int32),
            pltpu.SMEM((1, 1), jnp.int32),
            dma((6,)), pltpu.SemaphoreType.REGULAR((GROUPS - 2,)), dma, dma, dma, dma, dma((chunks,)), dma, dma((chunks,)),
        ],
        compiler_params=pltpu.CompilerParams(
            collective_id=0, has_side_effects=True, vmem_limit_bytes=32 * 1024 * 1024
        ),
        cost_estimate=pl.CostEstimate(flops=10**9, bytes_accessed=13 * 10**6, transcendentals=0),
    )(
        *(
            pltpu.with_memory_space_constraint(a, pltpu.HBM) if a.size > 1 else a
            for a in (
                block_ids, slot_counts, replica_deltas, replica_rows,
                outer_params.reshape(blocks, block, slab), momentum.reshape(blocks, block, slab),
            )
        ),
    )
    new_params, new_momentum, blended = pl.pallas_call(
        write_out,
        out_shape=results,
        in_specs=[vmem] * 3,
        out_specs=(hbm,) * 3,
        scratch_shapes=[dma((3,))],
        compiler_params=pltpu.CompilerParams(vmem_limit_bytes=16 * 1024 * 1024),
    )(*held)
    return new_params.reshape(outer_params.shape), new_momentum.reshape(momentum.shape), blended


def solution(mesh):
    in_specs = (
        P("expert", "replica"),
        P("expert", "replica"),
        P("replica", "expert", None, None),
        P("replica", "expert", None, None),
        P("replica", "expert"),
        P("replica", "expert"),
    )
    out_specs = (P("expert", "replica"), P("expert", "replica"), P("replica", "expert", None, None))
    return jax.shard_map(local, mesh=mesh, in_specs=in_specs, out_specs=out_specs, check_vma=False)
```

```python
import functools

import jax
import jax.numpy as jnp
from jax import lax
from jax.experimental import pallas as pl
from jax.experimental.pallas import tpu as pltpu
from jax.sharding import PartitionSpec as P

outer_rate = 0.7
nesterov_decay = 0.9
blend_weight = 0.5

MESH = pl.DeviceIdType.MESH
TILE = 16
LANES = 128
RING = 8


GROUPS = 5


def peer_in(g, i, me, n):
    if g == 0:
        dy, dz = i + 1, 0
    elif g == GROUPS - 1:
        dy, dz = i, g
    else:
        dy, dz = lax.div(i, 2), g * (1 - 2 * lax.rem(i, 2))
    z = lax.rem(lax.rem(me, RING) + dz + RING, RING)
    y = lax.rem(lax.div(me, RING) + dy, n // RING)
    return y * RING + z


def group_size(g, n):
    return (n // RING - 1, 2 * (n // RING), 2 * (n // RING), 2 * (n // RING), n // RING)[g]


def blend(rows, fetched, live):
    old = rows.astype(jnp.float32)
    mixed = blend_weight * old + (1.0 - blend_weight) * fetched.astype(jnp.float32)
    return jnp.where(live, mixed, old).astype(jnp.bfloat16)


def kernel(
    n, chunks, blocks,
    ids_ref, count_ref, deltas_ref, rows_ref, params_ref, momentum_ref,
    params, momentum, own, ret,
    src, got, sel, tally, fresh, back, mine, table, listed, own_ids, own_count,
    local_sem, known, table_sem, table_send, list_sem, send1, recv1, send2, recv2,
):
    me = lax.axis_index("replica")
    slots = src.shape[0]
    block = src.shape[1]
    rows = block // chunks
    tiles = rows // TILE
    total = n * slots
    parts = [pl.ds(c * rows, rows) for c in range(chunks)]
    pairs = (
        [(ids_ref, own_ids), (count_ref, own_count)]
        + [(deltas_ref.at[0, :, part], src.at[:, part]) for part in parts]
        + [(params_ref, params), (momentum_ref, momentum), (rows_ref, own)]
    )
    loads = [pltpu.make_async_copy(a, b, local_sem.at[i]) for i, (a, b) in enumerate(pairs)]
    urgent, deltas_loads, later = loads[:2], loads[2:-3], loads[-3:]

    barrier = pltpu.get_barrier_semaphore()

    for g in (0, 1):

        @pl.loop(0, group_size(g, n))
        def _(i):
            pl.semaphore_signal(
                barrier, inc=1, device_id={"replica": peer_in(g, i, me, n)}, device_id_type=MESH
            )

    for copy in urgent + deltas_loads:
        copy.start()
    for copy in urgent:
        copy.wait()
    first = lax.axis_index("expert") * blocks
    count = own_count[0, 0]
    lane = lax.broadcasted_iota(jnp.int32, (1, LANES), 1)
    row = jnp.full((1, LANES), -1, jnp.int32)
    for j in range(slots):
        row = jnp.where((lane == j) & (j < count), own_ids[0, j] - first, row)
    mine[...] = row
    table[me] = row
    deltas_loads[0].wait()
    pl.semaphore_wait(barrier, group_size(0, n) + group_size(1, n))

    def cols(p):
        return pl.ds(pl.multiple_of(p * LANES, LANES), LANES)

    def tell(level):
        for away in (1, RING - 1):
            z = lax.rem(lax.rem(me, RING) + away, RING)
            pl.semaphore_signal(
                known.at[level], inc=1, device_id={"replica": lax.div(me, RING) * RING + z}, device_id_type=MESH
            )

    def send_table(g):
        @pl.loop(0, group_size(g, n))
        def _(i):
            pltpu.make_async_remote_copy(
                src_ref=mine, dst_ref=table.at[me], send_sem=table_send, recv_sem=table_sem,
                device_id={"replica": peer_in(g, i, me, n)}, device_id_type=MESH,
            ).start()

    def send_slab(c, g):
        part = pl.ds(c * rows, rows)

        @pl.loop(0, group_size(g, n))
        def _(i):
            p = peer_in(g, i, me, n)
            pltpu.make_async_remote_copy(
                src_ref=src.at[:, part, cols(p)], dst_ref=got.at[c, me], send_sem=send1, recv_sem=recv1.at[c],
                device_id={"replica": p}, device_id_type=MESH,
            ).start()

    for g in range(GROUPS):
        if g > 1:
            pl.semaphore_wait(known.at[g - 2], 2)
        if 0 < g < GROUPS - 1:
            tell(g - 1)
        send_table(g)
        send_slab(0, g)

    for c in range(1, chunks):
        deltas_loads[c].wait()
        for g in range(GROUPS):
            send_slab(c, g)

    for copy in later:
        copy.start()
    for c in range(chunks):
        got[c, me] = src[:, c * rows : (c + 1) * rows, cols(me)]

    rest = table.at[pl.ds(0, n - 1)]
    pltpu.make_async_copy(rest, rest, table_sem).wait()
    to_scalars = pltpu.make_async_copy(table, listed, list_sem)
    to_scalars.start()
    to_scalars.wait()
    slot_of = lax.broadcasted_iota(jnp.int32, (1, total * TILE), 1)
    inner = lax.rem(slot_of, TILE)
    slot_of = lax.div(slot_of, TILE)
    target = jnp.full((1, total * TILE), -TILE, jnp.int32)
    for s in range(total):
        target = jnp.where(slot_of == s, listed[s // slots, 0, s % slots] * TILE, target)
    target = target + inner
    at = lax.broadcasted_iota(jnp.int32, (TILE, total * TILE), 0)

    @pl.loop(0, blocks)
    def _(b):
        there = pl.ds(pl.multiple_of(b * TILE, TILE), TILE)
        sel[there, :] = jnp.where(at + b * TILE == target, 1.0, 0.0).astype(jnp.bfloat16)

    tally[...] = jnp.maximum(
        jnp.dot(sel[...], jnp.ones((total * TILE, LANES), jnp.bfloat16), preferred_element_type=jnp.float32), 1.0
    )
    later[0].wait()
    later[1].wait()

    @pl.loop(0, chunks)
    def _(c):
        arrived = got.at[c, pl.ds(0, n - 1)]
        pltpu.make_async_copy(arrived, arrived, recv1.at[c]).wait()

        @pl.loop(0, tiles)
        def _(t):
            inside = pl.ds(pl.multiple_of(t * TILE, TILE), TILE)
            here = pl.ds(pl.multiple_of(c * rows + t * TILE, TILE), TILE)
            tile = got[c, :, :, inside, :].reshape(total * TILE, LANES)
            totals = jnp.dot(sel[...], tile, preferred_element_type=jnp.float32)
            mean = totals / tally[...]
            moment = nesterov_decay * momentum[:, here, :].reshape(blocks * TILE, LANES).astype(jnp.float32) + mean
            fresh_tile = params[:, here, :].reshape(blocks * TILE, LANES) - outer_rate * (
                mean + nesterov_decay * moment
            )
            params[:, here, :] = fresh_tile.reshape(blocks, TILE, LANES)
            momentum[:, here, :] = moment.astype(jnp.bfloat16).reshape(blocks, TILE, LANES)
            fresh[:, inside, :] = fresh_tile.astype(jnp.bfloat16).reshape(blocks, TILE, LANES)

        part = pl.ds(pl.multiple_of(c * rows, TILE), rows)
        for s in range(total):
            back[c, s // slots, s % slots] = fresh[jnp.maximum(listed[s // slots, 0, s % slots], 0)]

        for j in range(slots):
            ret[j, part, cols(me)] = fresh[jnp.maximum(listed[me, 0, j], 0)]

        def send_back(g, wanted):
            @pl.loop(0, group_size(g, n))
            def _(i):
                p = peer_in(g, i, me, n)

                @pl.when(wanted(lax.rem(p, RING)))
                def _():
                    pltpu.make_async_remote_copy(
                        src_ref=back.at[c, p], dst_ref=ret.at[:, part, cols(me)], send_sem=send2,
                        recv_sem=recv2.at[c], device_id={"replica": p}, device_id_type=MESH,
                    ).start()

        for low, high in ((0, 1), (1, 2), (2, 3), (3, 4), (4, 8)):
            for g in reversed(range(GROUPS)):
                send_back(g, lambda z: (low <= z) & (z < high))

    later[2].wait()

    def wait_back(c):
        arrived = got.at[c, pl.ds(0, n - 1)]
        pltpu.make_async_copy(arrived, arrived, recv2.at[c]).wait()

    @pl.loop(0, chunks - 1)
    def _(c):
        wait_back(c)
        part = pl.ds(pl.multiple_of(c * rows, TILE), rows)
        for j in range(slots):

            @pl.loop(0, n)
            def _(q):
                own[0, j, part, cols(q)] = blend(own[0, j, part, cols(q)], ret[j, part, cols(q)], j < count)

    wait_back(chunks - 1)
    pltpu.make_async_copy(rest, rest, table_send).wait()
    sent = got.at[:, pl.ds(0, n - 1)]
    pltpu.make_async_copy(sent, sent, send1).wait()
    pltpu.make_async_copy(sent, sent, send2).wait()


def write_out(
    start, pieces, count_ref, params, momentum, own, ret, params_out, momentum_out, blended_out, mixed, sem
):
    count = count_ref[0, 0]
    done = [pltpu.make_async_copy(params, params_out, sem.at[0]), pltpu.make_async_copy(momentum, momentum_out, sem.at[1])]
    if start:
        ready = pl.ds(0, start)
        done.append(pltpu.make_async_copy(own.at[:, :, ready], blended_out.at[:, :, ready], sem.at[2]))
    for copy in done:
        copy.start()
    slots, block, width = own.shape[1:]
    rows = (block - start) // pieces
    for p in range(pieces):
        for j in range(slots):
            here = pl.ds(start + p * rows, rows)
            there = pl.ds(p * rows, rows)

            @pl.loop(0, width // LANES)
            def _(q):
                at = pl.ds(pl.multiple_of(q * LANES, LANES), LANES)
                mixed[j, there, at] = blend(own[0, j, here, at], ret[j, here, at], j < count)

            copy = pltpu.make_async_copy(mixed.at[j, there], blended_out.at[0, j, here], sem.at[3 + p * slots + j])
            copy.start()
            done.append(copy)
    for copy in done:
        copy.wait()


def local(outer_params, momentum, replica_deltas, replica_rows, block_ids, slot_counts):
    n = lax.axis_size("replica")
    _, slots, block, width = replica_deltas.shape
    blocks = outer_params.shape[0] // block
    slab = outer_params.shape[1]
    total = n * slots
    chunks = 2
    pieces = 2
    rows = block // chunks
    f32, bf16 = jnp.float32, jnp.bfloat16
    hbm = pl.BlockSpec(memory_space=pltpu.HBM)
    vmem = pl.BlockSpec(memory_space=pltpu.VMEM)
    dma = pltpu.SemaphoreType.DMA
    results = (
        jax.ShapeDtypeStruct((blocks, block, slab), f32),
        jax.ShapeDtypeStruct((blocks, block, slab), bf16),
        jax.ShapeDtypeStruct(replica_rows.shape, bf16),
    )
    held = pl.pallas_call(
        functools.partial(kernel, n, chunks, blocks),
        out_shape=results + (jax.ShapeDtypeStruct((slots, block, width), bf16),),
        in_specs=[hbm] * 6,
        out_specs=(vmem,) * 4,
        scratch_shapes=[
            pltpu.VMEM((slots, block, width), bf16),
            pltpu.VMEM((chunks, n, slots, rows, slab), bf16),
            pltpu.VMEM((blocks * TILE, total * TILE), bf16),
            pltpu.VMEM((blocks * TILE, slab), f32),
            pltpu.VMEM((blocks, rows, slab), bf16),
            pltpu.VMEM((chunks, n, slots, rows, slab), bf16),
            pltpu.VMEM((1, LANES), jnp.int32),
            pltpu.VMEM((n, 1, LANES), jnp.int32),
            pltpu.SMEM((n, 1, LANES), jnp.int32),
            pltpu.SMEM((1, slots), jnp.int32),
            pltpu.SMEM((1, 1), jnp.int32),
            dma((5 + chunks,)), pltpu.SemaphoreType.REGULAR((GROUPS - 2,)), dma, dma, dma, dma, dma((chunks,)), dma, dma((chunks,)),
        ],
        compiler_params=pltpu.CompilerParams(
            collective_id=0, has_side_effects=True, vmem_limit_bytes=32 * 1024 * 1024
        ),
        cost_estimate=pl.CostEstimate(flops=10**9, bytes_accessed=13 * 10**6, transcendentals=0),
    )(
        *(
            pltpu.with_memory_space_constraint(a, pltpu.HBM) if a.size > 1 else a
            for a in (
                block_ids, slot_counts, replica_deltas, replica_rows,
                outer_params.reshape(blocks, block, slab), momentum.reshape(blocks, block, slab),
            )
        ),
    )
    new_params, new_momentum, blended = pl.pallas_call(
        functools.partial(write_out, block - rows, pieces),
        out_shape=results,
        in_specs=[pl.BlockSpec(memory_space=pltpu.SMEM)] + [vmem] * 4,
        out_specs=(hbm,) * 3,
        scratch_shapes=[pltpu.VMEM((slots, rows, width), bf16), dma((3 + slots * pieces,))],
        compiler_params=pltpu.CompilerParams(vmem_limit_bytes=16 * 1024 * 1024),
    )(slot_counts, *held)
    return new_params.reshape(outer_params.shape), new_momentum.reshape(momentum.shape), blended


def solution(mesh):
    in_specs = (
        P("expert", "replica"),
        P("expert", "replica"),
        P("replica", "expert", None, None),
        P("replica", "expert", None, None),
        P("replica", "expert"),
        P("replica", "expert"),
    )
    out_specs = (P("expert", "replica"), P("expert", "replica"), P("replica", "expert", None, None))
    return jax.shard_map(local, mesh=mesh, in_specs=in_specs, out_specs=out_specs, check_vma=False)
```

```python
import functools

import jax
import jax.numpy as jnp
from jax import lax
from jax.experimental import pallas as pl
from jax.experimental.pallas import tpu as pltpu
from jax.sharding import PartitionSpec as P

outer_rate = 0.7
nesterov_decay = 0.9
blend_weight = 0.5

MESH = pl.DeviceIdType.MESH
TILE = 16
LANES = 128
RING = 8


GROUPS = 5


def peer_in(g, i, me, n):
    if g == 0:
        dy, dz = i + 1, 0
    elif g == GROUPS - 1:
        dy, dz = i, g
    else:
        dy, dz = lax.div(i, 2), g * (1 - 2 * lax.rem(i, 2))
    z = lax.rem(lax.rem(me, RING) + dz + RING, RING)
    y = lax.rem(lax.div(me, RING) + dy, n // RING)
    return y * RING + z


def group_size(g, n):
    return (n // RING - 1, 2 * (n // RING), 2 * (n // RING), 2 * (n // RING), n // RING)[g]


def blend(rows, fetched, live):
    old = rows.astype(jnp.float32)
    mixed = blend_weight * old + (1.0 - blend_weight) * fetched.astype(jnp.float32)
    return jnp.where(live, mixed, old).astype(jnp.bfloat16)


def kernel(
    n, chunks, blocks,
    ids_ref, count_ref, deltas_ref, rows_ref, params_ref, momentum_ref,
    params, momentum, own, ret,
    src, got, sel, tally, fresh, back, mine, table, listed, own_ids, own_count,
    local_sem, known, table_sem, table_send, list_sem, send1, recv1, send2, recv2,
):
    me = lax.axis_index("replica")
    slots = src.shape[0]
    block = src.shape[1]
    rows = block // chunks
    tiles = rows // TILE
    total = n * slots
    parts = [pl.ds(c * rows, rows) for c in range(chunks)]
    pairs = (
        [(ids_ref, own_ids), (count_ref, own_count)]
        + [(deltas_ref.at[0, :, part], src.at[:, part]) for part in parts]
        + [(params_ref, params), (momentum_ref, momentum), (rows_ref, own)]
    )
    loads = [pltpu.make_async_copy(a, b, local_sem.at[i]) for i, (a, b) in enumerate(pairs)]
    urgent, deltas_loads, later = loads[:2], loads[2:-3], loads[-3:]

    barrier = pltpu.get_barrier_semaphore()

    for g in (0, 1):

        @pl.loop(0, group_size(g, n))
        def _(i):
            pl.semaphore_signal(
                barrier, inc=1, device_id={"replica": peer_in(g, i, me, n)}, device_id_type=MESH
            )

    for copy in urgent + deltas_loads:
        copy.start()
    for copy in urgent:
        copy.wait()
    first = lax.axis_index("expert") * blocks
    count = own_count[0, 0]
    lane = lax.broadcasted_iota(jnp.int32, (1, LANES), 1)
    row = jnp.full((1, LANES), -1, jnp.int32)
    for j in range(slots):
        row = jnp.where((lane == j) & (j < count), own_ids[0, j] - first, row)
    mine[...] = row
    table[me] = row
    deltas_loads[0].wait()
    pl.semaphore_wait(barrier, group_size(0, n) + group_size(1, n))

    def cols(p):
        return pl.ds(pl.multiple_of(p * LANES, LANES), LANES)

    def tell(level):
        for away in (1, RING - 1):
            z = lax.rem(lax.rem(me, RING) + away, RING)
            pl.semaphore_signal(
                known.at[level], inc=1, device_id={"replica": lax.div(me, RING) * RING + z}, device_id_type=MESH
            )

    def send_table(g):
        @pl.loop(0, group_size(g, n))
        def _(i):
            pltpu.make_async_remote_copy(
                src_ref=mine, dst_ref=table.at[me], send_sem=table_send, recv_sem=table_sem,
                device_id={"replica": peer_in(g, i, me, n)}, device_id_type=MESH,
            ).start()

    def send_slab(c, g):
        part = pl.ds(c * rows, rows)

        @pl.loop(0, group_size(g, n))
        def _(i):
            p = peer_in(g, i, me, n)
            pltpu.make_async_remote_copy(
                src_ref=src.at[:, part, cols(p)], dst_ref=got.at[c, me], send_sem=send1, recv_sem=recv1.at[c],
                device_id={"replica": p}, device_id_type=MESH,
            ).start()

    for g in range(GROUPS):
        if g > 1:
            pl.semaphore_wait(known.at[g - 2], 2)
        if 0 < g < GROUPS - 1:
            tell(g - 1)
        send_table(g)
        send_slab(0, g)

    for c in range(1, chunks):
        deltas_loads[c].wait()
        for g in range(GROUPS):
            send_slab(c, g)

    for copy in later:
        copy.start()
    for c in range(chunks):
        got[c, me] = src[:, c * rows : (c + 1) * rows, cols(me)]

    rest = table.at[pl.ds(0, n - 1)]
    pltpu.make_async_copy(rest, rest, table_sem).wait()
    to_scalars = pltpu.make_async_copy(table, listed, list_sem)
    to_scalars.start()
    to_scalars.wait()
    slot_of = lax.broadcasted_iota(jnp.int32, (1, total * TILE), 1)
    inner = lax.rem(slot_of, TILE)
    slot_of = lax.div(slot_of, TILE)
    target = jnp.full((1, total * TILE), -TILE, jnp.int32)
    for s in range(total):
        target = jnp.where(slot_of == s, listed[s // slots, 0, s % slots] * TILE, target)
    target = target + inner
    at = lax.broadcasted_iota(jnp.int32, (TILE, total * TILE), 0)

    @pl.loop(0, blocks)
    def _(b):
        there = pl.ds(pl.multiple_of(b * TILE, TILE), TILE)
        sel[there, :] = jnp.where(at + b * TILE == target, 1.0, 0.0).astype(jnp.bfloat16)

    tally[...] = jnp.maximum(
        jnp.dot(sel[...], jnp.ones((total * TILE, LANES), jnp.bfloat16), preferred_element_type=jnp.float32), 1.0
    )
    later[0].wait()
    later[1].wait()

    @pl.loop(0, chunks)
    def _(c):
        arrived = got.at[c, pl.ds(0, n - 1)]
        pltpu.make_async_copy(arrived, arrived, recv1.at[c]).wait()

        @pl.loop(0, tiles)
        def _(t):
            inside = pl.ds(pl.multiple_of(t * TILE, TILE), TILE)
            here = pl.ds(pl.multiple_of(c * rows + t * TILE, TILE), TILE)
            tile = got[c, :, :, inside, :].reshape(total * TILE, LANES)
            totals = jnp.dot(sel[...], tile, preferred_element_type=jnp.float32)
            mean = totals / tally[...]
            moment = nesterov_decay * momentum[:, here, :].reshape(blocks * TILE, LANES).astype(jnp.float32) + mean
            fresh_tile = params[:, here, :].reshape(blocks * TILE, LANES) - outer_rate * (
                mean + nesterov_decay * moment
            )
            params[:, here, :] = fresh_tile.reshape(blocks, TILE, LANES)
            momentum[:, here, :] = moment.astype(jnp.bfloat16).reshape(blocks, TILE, LANES)
            fresh[:, inside, :] = fresh_tile.astype(jnp.bfloat16).reshape(blocks, TILE, LANES)

        part = pl.ds(pl.multiple_of(c * rows, TILE), rows)
        for s in range(total):
            back[c, s // slots, s % slots] = fresh[jnp.maximum(listed[s // slots, 0, s % slots], 0)]

        for j in range(slots):
            ret[j, part, cols(me)] = fresh[jnp.maximum(listed[me, 0, j], 0)]

        def send_back(g, wanted):
            @pl.loop(0, group_size(g, n))
            def _(i):
                p = peer_in(g, i, me, n)

                @pl.when(wanted(lax.rem(p, RING), lax.div(p, RING)))
                def _():
                    pltpu.make_async_remote_copy(
                        src_ref=back.at[c, p], dst_ref=ret.at[:, part, cols(me)], send_sem=send2,
                        recv_sem=recv2.at[c], device_id={"replica": p}, device_id_type=MESH,
                    ).start()

        for low, high in ((0, 1), (1, 2), (2, 3), (3, 4), (4, RING)):
            for start, stop in ((0, 1), (1, n // RING)) if high <= RING // 2 else ((0, n // RING),):
                for g in reversed(range(GROUPS)):
                    send_back(g, lambda z, y: (low <= z) & (z < high) & (start <= y) & (y < stop))

    later[2].wait()

    def wait_back(c):
        arrived = got.at[c, pl.ds(0, n - 1)]
        pltpu.make_async_copy(arrived, arrived, recv2.at[c]).wait()

    @pl.loop(0, chunks - 1)
    def _(c):
        wait_back(c)
        part = pl.ds(pl.multiple_of(c * rows, TILE), rows)
        for j in range(slots):

            @pl.loop(0, n)
            def _(q):
                own[0, j, part, cols(q)] = blend(own[0, j, part, cols(q)], ret[j, part, cols(q)], j < count)

    wait_back(chunks - 1)
    pltpu.make_async_copy(rest, rest, table_send).wait()
    sent = got.at[:, pl.ds(0, n - 1)]
    pltpu.make_async_copy(sent, sent, send1).wait()
    pltpu.make_async_copy(sent, sent, send2).wait()


def write_out(
    start, pieces, count_ref, params, momentum, own, ret, params_out, momentum_out, blended_out, mixed, sem
):
    count = count_ref[0, 0]
    done = [pltpu.make_async_copy(params, params_out, sem.at[0]), pltpu.make_async_copy(momentum, momentum_out, sem.at[1])]
    if start:
        ready = pl.ds(0, start)
        done.append(pltpu.make_async_copy(own.at[:, :, ready], blended_out.at[:, :, ready], sem.at[2]))
    for copy in done:
        copy.start()
    slots, block, width = own.shape[1:]
    rows = (block - start) // pieces
    for p in range(pieces):
        for j in range(slots):
            here = pl.ds(start + p * rows, rows)
            there = pl.ds(p * rows, rows)

            @pl.loop(0, width // LANES)
            def _(q):
                at = pl.ds(pl.multiple_of(q * LANES, LANES), LANES)
                mixed[j, there, at] = blend(own[0, j, here, at], ret[j, here, at], j < count)

            copy = pltpu.make_async_copy(mixed.at[j, there], blended_out.at[0, j, here], sem.at[3 + p * slots + j])
            copy.start()
            done.append(copy)
    for copy in done:
        copy.wait()


def local(outer_params, momentum, replica_deltas, replica_rows, block_ids, slot_counts):
    n = lax.axis_size("replica")
    _, slots, block, width = replica_deltas.shape
    blocks = outer_params.shape[0] // block
    slab = outer_params.shape[1]
    total = n * slots
    chunks = 2
    pieces = 2
    rows = block // chunks
    f32, bf16 = jnp.float32, jnp.bfloat16
    hbm = pl.BlockSpec(memory_space=pltpu.HBM)
    vmem = pl.BlockSpec(memory_space=pltpu.VMEM)
    dma = pltpu.SemaphoreType.DMA
    results = (
        jax.ShapeDtypeStruct((blocks, block, slab), f32),
        jax.ShapeDtypeStruct((blocks, block, slab), bf16),
        jax.ShapeDtypeStruct(replica_rows.shape, bf16),
    )
    held = pl.pallas_call(
        functools.partial(kernel, n, chunks, blocks),
        out_shape=results + (jax.ShapeDtypeStruct((slots, block, width), bf16),),
        in_specs=[hbm] * 6,
        out_specs=(vmem,) * 4,
        scratch_shapes=[
            pltpu.VMEM((slots, block, width), bf16),
            pltpu.VMEM((chunks, n, slots, rows, slab), bf16),
            pltpu.VMEM((blocks * TILE, total * TILE), bf16),
            pltpu.VMEM((blocks * TILE, slab), f32),
            pltpu.VMEM((blocks, rows, slab), bf16),
            pltpu.VMEM((chunks, n, slots, rows, slab), bf16),
            pltpu.VMEM((1, LANES), jnp.int32),
            pltpu.VMEM((n, 1, LANES), jnp.int32),
            pltpu.SMEM((n, 1, LANES), jnp.int32),
            pltpu.SMEM((1, slots), jnp.int32),
            pltpu.SMEM((1, 1), jnp.int32),
            dma((5 + chunks,)), pltpu.SemaphoreType.REGULAR((GROUPS - 2,)), dma, dma, dma, dma, dma((chunks,)), dma, dma((chunks,)),
        ],
        compiler_params=pltpu.CompilerParams(
            collective_id=0, has_side_effects=True, vmem_limit_bytes=32 * 1024 * 1024
        ),
        cost_estimate=pl.CostEstimate(flops=10**9, bytes_accessed=13 * 10**6, transcendentals=0),
    )(
        *(
            pltpu.with_memory_space_constraint(a, pltpu.HBM) if a.size > 1 else a
            for a in (
                block_ids, slot_counts, replica_deltas, replica_rows,
                outer_params.reshape(blocks, block, slab), momentum.reshape(blocks, block, slab),
            )
        ),
    )
    new_params, new_momentum, blended = pl.pallas_call(
        functools.partial(write_out, block - rows, pieces),
        out_shape=results,
        in_specs=[pl.BlockSpec(memory_space=pltpu.SMEM)] + [vmem] * 4,
        out_specs=(hbm,) * 3,
        scratch_shapes=[pltpu.VMEM((slots, rows, width), bf16), dma((3 + slots * pieces,))],
        compiler_params=pltpu.CompilerParams(vmem_limit_bytes=16 * 1024 * 1024),
    )(slot_counts, *held)
    return new_params.reshape(outer_params.shape), new_momentum.reshape(momentum.shape), blended


def solution(mesh):
    in_specs = (
        P("expert", "replica"),
        P("expert", "replica"),
        P("replica", "expert", None, None),
        P("replica", "expert", None, None),
        P("replica", "expert"),
        P("replica", "expert"),
    )
    out_specs = (P("expert", "replica"), P("expert", "replica"), P("replica", "expert", None, None))
    return jax.shard_map(local, mesh=mesh, in_specs=in_specs, out_specs=out_specs, check_vma=False)
```

```python
import functools

import jax
import jax.numpy as jnp
from jax import lax
from jax.experimental import pallas as pl
from jax.experimental.pallas import tpu as pltpu
from jax.sharding import PartitionSpec as P

outer_rate = 0.7
nesterov_decay = 0.9
blend_weight = 0.5

MESH = pl.DeviceIdType.MESH
TILE = 16
LANES = 128
RING = 8


GROUPS = 5


def peer_in(g, i, me, n):
    if g == 0:
        dy, dz = i + 1, 0
    elif g == GROUPS - 1:
        dy, dz = i, g
    else:
        dy, dz = lax.div(i, 2), g * (1 - 2 * lax.rem(i, 2))
    z = lax.rem(lax.rem(me, RING) + dz + RING, RING)
    y = lax.rem(lax.div(me, RING) + dy, n // RING)
    return y * RING + z


def group_size(g, n):
    return (n // RING - 1, 2 * (n // RING), 2 * (n // RING), 2 * (n // RING), n // RING)[g]


def blend(rows, fetched, live):
    old = rows.astype(jnp.float32)
    mixed = blend_weight * old + (1.0 - blend_weight) * fetched.astype(jnp.float32)
    return jnp.where(live, mixed, old).astype(jnp.bfloat16)


def kernel(
    n, chunks, blocks,
    ids_ref, count_ref, deltas_ref, rows_ref, params_ref, momentum_ref,
    params, momentum, own, ret,
    src, got, sel, tally, fresh, back, mine, table, listed, own_ids, own_count,
    local_sem, known, table_sem, table_send, list_sem, send1, recv1, send2, recv2,
):
    me = lax.axis_index("replica")
    slots = src.shape[0]
    block = src.shape[1]
    rows = block // chunks
    tiles = rows // TILE
    total = n * slots
    parts = [pl.ds(c * rows, rows) for c in range(chunks)]
    pairs = (
        [(ids_ref, own_ids), (count_ref, own_count)]
        + [(deltas_ref.at[0, :, part], src.at[:, part]) for part in parts]
        + [(params_ref, params), (momentum_ref, momentum), (rows_ref, own)]
    )
    loads = [pltpu.make_async_copy(a, b, local_sem.at[i]) for i, (a, b) in enumerate(pairs)]
    urgent, deltas_loads, later = loads[:2], loads[2:-3], loads[-3:]

    barrier = pltpu.get_barrier_semaphore()

    for g in (0, 1):

        @pl.loop(0, group_size(g, n))
        def _(i):
            pl.semaphore_signal(
                barrier, inc=1, device_id={"replica": peer_in(g, i, me, n)}, device_id_type=MESH
            )

    for copy in urgent + deltas_loads:
        copy.start()
    for copy in urgent:
        copy.wait()
    first = lax.axis_index("expert") * blocks
    count = own_count[0, 0]
    lane = lax.broadcasted_iota(jnp.int32, (1, LANES), 1)
    row = jnp.full((1, LANES), -1, jnp.int32)
    for j in range(slots):
        row = jnp.where((lane == j) & (j < count), own_ids[0, j] - first, row)
    mine[...] = row
    table[me] = row
    deltas_loads[0].wait()
    pl.semaphore_wait(barrier, group_size(0, n) + group_size(1, n))

    def cols(p):
        return pl.ds(pl.multiple_of(p * LANES, LANES), LANES)

    def tell(level):
        for away in (1, RING - 1):
            z = lax.rem(lax.rem(me, RING) + away, RING)
            pl.semaphore_signal(
                known.at[level], inc=1, device_id={"replica": lax.div(me, RING) * RING + z}, device_id_type=MESH
            )

    def send_table(g):
        @pl.loop(0, group_size(g, n))
        def _(i):
            pltpu.make_async_remote_copy(
                src_ref=mine, dst_ref=table.at[me], send_sem=table_send, recv_sem=table_sem,
                device_id={"replica": peer_in(g, i, me, n)}, device_id_type=MESH,
            ).start()

    def send_slab(c, g):
        part = pl.ds(c * rows, rows)

        @pl.loop(0, group_size(g, n))
        def _(i):
            p = peer_in(g, i, me, n)
            pltpu.make_async_remote_copy(
                src_ref=src.at[:, part, cols(p)], dst_ref=got.at[c, me], send_sem=send1, recv_sem=recv1.at[c],
                device_id={"replica": p}, device_id_type=MESH,
            ).start()

    for g in range(GROUPS):
        if g > 1:
            pl.semaphore_wait(known.at[g - 2], 2)
        if 0 < g < GROUPS - 1:
            tell(g - 1)
        send_table(g)
        send_slab(0, g)

    for c in range(1, chunks):
        deltas_loads[c].wait()
        for g in range(GROUPS):
            send_slab(c, g)

    for copy in later:
        copy.start()
    for c in range(chunks):
        got[c, me] = src[:, c * rows : (c + 1) * rows, cols(me)]

    rest = table.at[pl.ds(0, n - 1)]
    pltpu.make_async_copy(rest, rest, table_sem).wait()
    to_scalars = pltpu.make_async_copy(table, listed, list_sem)
    to_scalars.start()
    to_scalars.wait()
    slot_of = lax.broadcasted_iota(jnp.int32, (1, total * TILE), 1)
    inner = lax.rem(slot_of, TILE)
    slot_of = lax.div(slot_of, TILE)
    target = jnp.full((1, total * TILE), -TILE, jnp.int32)
    for s in range(total):
        target = jnp.where(slot_of == s, listed[s // slots, 0, s % slots] * TILE, target)
    target = target + inner
    at = lax.broadcasted_iota(jnp.int32, (TILE, total * TILE), 0)

    @pl.loop(0, blocks)
    def _(b):
        there = pl.ds(pl.multiple_of(b * TILE, TILE), TILE)
        sel[there, :] = jnp.where(at + b * TILE == target, 1.0, 0.0).astype(jnp.bfloat16)

    tally[...] = jnp.maximum(
        jnp.dot(sel[...], jnp.ones((total * TILE, LANES), jnp.bfloat16), preferred_element_type=jnp.float32), 1.0
    )
    later[0].wait()
    later[1].wait()

    @pl.loop(0, chunks)
    def _(c):
        arrived = got.at[c, pl.ds(0, n - 1)]
        pltpu.make_async_copy(arrived, arrived, recv1.at[c]).wait()

        @pl.loop(0, tiles)
        def _(t):
            inside = pl.ds(pl.multiple_of(t * TILE, TILE), TILE)
            here = pl.ds(pl.multiple_of(c * rows + t * TILE, TILE), TILE)
            tile = got[c, :, :, inside, :].reshape(total * TILE, LANES)
            totals = jnp.dot(sel[...], tile, preferred_element_type=jnp.float32)
            mean = totals / tally[...]
            moment = nesterov_decay * momentum[:, here, :].reshape(blocks * TILE, LANES).astype(jnp.float32) + mean
            fresh_tile = params[:, here, :].reshape(blocks * TILE, LANES) - outer_rate * (
                mean + nesterov_decay * moment
            )
            params[:, here, :] = fresh_tile.reshape(blocks, TILE, LANES)
            momentum[:, here, :] = moment.astype(jnp.bfloat16).reshape(blocks, TILE, LANES)
            fresh[:, inside, :] = fresh_tile.astype(jnp.bfloat16).reshape(blocks, TILE, LANES)

        part = pl.ds(pl.multiple_of(c * rows, TILE), rows)
        for s in range(total):
            back[c, s // slots, s % slots] = fresh[jnp.maximum(listed[s // slots, 0, s % slots], 0)]

        for j in range(slots):
            ret[j, part, cols(me)] = fresh[jnp.maximum(listed[me, 0, j], 0)]

        def send_back(g, wanted):
            @pl.loop(0, group_size(g, n))
            def _(i):
                p = peer_in(g, i, me, n)

                @pl.when(wanted(lax.rem(p, RING), lax.div(p, RING)))
                def _():
                    pltpu.make_async_remote_copy(
                        src_ref=back.at[c, p], dst_ref=ret.at[:, part, cols(me)], send_sem=send2,
                        recv_sem=recv2.at[c], device_id={"replica": p}, device_id_type=MESH,
                    ).start()

        y_all = n // RING
        classes = (
            (0, 1, 0, 1), (0, 1, 1, y_all), (2, 3, 0, 2), (1, 2, 0, 1), (1, 2, 1, y_all), (2, 3, 2, y_all),
            (3, 4, 0, 1), (3, 4, 1, y_all), (4, RING, 0, y_all),
        )
        for low, high, start, stop in classes:
            for g in reversed(range(GROUPS)):
                send_back(g, lambda z, y: (low <= z) & (z < high) & (start <= y) & (y < stop))

    later[2].wait()

    def wait_back(c):
        arrived = got.at[c, pl.ds(0, n - 1)]
        pltpu.make_async_copy(arrived, arrived, recv2.at[c]).wait()

    @pl.loop(0, chunks - 1)
    def _(c):
        wait_back(c)
        part = pl.ds(pl.multiple_of(c * rows, TILE), rows)
        for j in range(slots):

            @pl.loop(0, n)
            def _(q):
                own[0, j, part, cols(q)] = blend(own[0, j, part, cols(q)], ret[j, part, cols(q)], j < count)

    wait_back(chunks - 1)
    pltpu.make_async_copy(rest, rest, table_send).wait()
    sent = got.at[:, pl.ds(0, n - 1)]
    pltpu.make_async_copy(sent, sent, send1).wait()
    pltpu.make_async_copy(sent, sent, send2).wait()


def write_out(
    start, pieces, count_ref, params, momentum, own, ret, params_out, momentum_out, blended_out, mixed, sem
):
    count = count_ref[0, 0]
    done = [pltpu.make_async_copy(params, params_out, sem.at[0]), pltpu.make_async_copy(momentum, momentum_out, sem.at[1])]
    if start:
        ready = pl.ds(0, start)
        done.append(pltpu.make_async_copy(own.at[:, :, ready], blended_out.at[:, :, ready], sem.at[2]))
    for copy in done:
        copy.start()
    slots, block, width = own.shape[1:]
    rows = (block - start) // pieces
    for p in range(pieces):
        for j in range(slots):
            here = pl.ds(start + p * rows, rows)
            there = pl.ds(p * rows, rows)

            @pl.loop(0, width // LANES)
            def _(q):
                at = pl.ds(pl.multiple_of(q * LANES, LANES), LANES)
                mixed[j, there, at] = blend(own[0, j, here, at], ret[j, here, at], j < count)

            copy = pltpu.make_async_copy(mixed.at[j, there], blended_out.at[0, j, here], sem.at[3 + p * slots + j])
            copy.start()
            done.append(copy)
    for copy in done:
        copy.wait()


def local(outer_params, momentum, replica_deltas, replica_rows, block_ids, slot_counts):
    n = lax.axis_size("replica")
    _, slots, block, width = replica_deltas.shape
    blocks = outer_params.shape[0] // block
    slab = outer_params.shape[1]
    total = n * slots
    chunks = 2
    pieces = 2
    rows = block // chunks
    f32, bf16 = jnp.float32, jnp.bfloat16
    hbm = pl.BlockSpec(memory_space=pltpu.HBM)
    vmem = pl.BlockSpec(memory_space=pltpu.VMEM)
    dma = pltpu.SemaphoreType.DMA
    results = (
        jax.ShapeDtypeStruct((blocks, block, slab), f32),
        jax.ShapeDtypeStruct((blocks, block, slab), bf16),
        jax.ShapeDtypeStruct(replica_rows.shape, bf16),
    )
    held = pl.pallas_call(
        functools.partial(kernel, n, chunks, blocks),
        out_shape=results + (jax.ShapeDtypeStruct((slots, block, width), bf16),),
        in_specs=[hbm] * 6,
        out_specs=(vmem,) * 4,
        scratch_shapes=[
            pltpu.VMEM((slots, block, width), bf16),
            pltpu.VMEM((chunks, n, slots, rows, slab), bf16),
            pltpu.VMEM((blocks * TILE, total * TILE), bf16),
            pltpu.VMEM((blocks * TILE, slab), f32),
            pltpu.VMEM((blocks, rows, slab), bf16),
            pltpu.VMEM((chunks, n, slots, rows, slab), bf16),
            pltpu.VMEM((1, LANES), jnp.int32),
            pltpu.VMEM((n, 1, LANES), jnp.int32),
            pltpu.SMEM((n, 1, LANES), jnp.int32),
            pltpu.SMEM((1, slots), jnp.int32),
            pltpu.SMEM((1, 1), jnp.int32),
            dma((5 + chunks,)), pltpu.SemaphoreType.REGULAR((GROUPS - 2,)), dma, dma, dma, dma, dma((chunks,)), dma, dma((chunks,)),
        ],
        compiler_params=pltpu.CompilerParams(
            collective_id=0, has_side_effects=True, vmem_limit_bytes=32 * 1024 * 1024
        ),
        cost_estimate=pl.CostEstimate(flops=10**9, bytes_accessed=13 * 10**6, transcendentals=0),
    )(
        *(
            pltpu.with_memory_space_constraint(a, pltpu.HBM) if a.size > 1 else a
            for a in (
                block_ids, slot_counts, replica_deltas, replica_rows,
                outer_params.reshape(blocks, block, slab), momentum.reshape(blocks, block, slab),
            )
        ),
    )
    new_params, new_momentum, blended = pl.pallas_call(
        functools.partial(write_out, block - rows, pieces),
        out_shape=results,
        in_specs=[pl.BlockSpec(memory_space=pltpu.SMEM)] + [vmem] * 4,
        out_specs=(hbm,) * 3,
        scratch_shapes=[pltpu.VMEM((slots, rows, width), bf16), dma((3 + slots * pieces,))],
        compiler_params=pltpu.CompilerParams(vmem_limit_bytes=16 * 1024 * 1024),
    )(slot_counts, *held)
    return new_params.reshape(outer_params.shape), new_momentum.reshape(momentum.shape), blended


def solution(mesh):
    in_specs = (
        P("expert", "replica"),
        P("expert", "replica"),
        P("replica", "expert", None, None),
        P("replica", "expert", None, None),
        P("replica", "expert"),
        P("replica", "expert"),
    )
    out_specs = (P("expert", "replica"), P("expert", "replica"), P("replica", "expert", None, None))
    return jax.shard_map(local, mesh=mesh, in_specs=in_specs, out_specs=out_specs, check_vma=False)
```
